128 devices in a mesh: layer: 32 (over x_hi, y, z), cuts: 4 (over x_lo, core).
Axes of the slice: x: 4 (x_hi: 2, x_lo: 2; x = x_hi * 2 + x_lo), y: 4, z: 4, core: 2. Of those that a mesh axis runs over, the one named last changes fastest.
Arguments:
- resid: bfloat16 [512, 2, 16384], P(None, None, 'cuts'), may hold values from -6 to 6
- enc_weight: bfloat16 [2, 16384, 8192], P(None, 'cuts', 'layer'), may hold values from -0.03125 to 0.03125
- enc_bias: float32 [8192], P('layer'), may hold values from -1 to 1
- dec_weight: bfloat16 [8192, 2, 16384], P('layer', None, 'cuts'), may hold values from -0.09375 to 0.09375
- dec_bias: float32 [2, 16384], P(None, 'cuts'), may hold values from -1 to 1
Outputs:
- enc_grad: bfloat16 [2, 16384, 8192], P(None, 'cuts', 'layer')
- dec_grad: bfloat16 [8192, 2, 16384], P('layer', None, 'cuts')
The draws below stay inside these ranges and needn't reach their ends.
All inputs are finite; a program needn't handle non-finite values.
Results may differ from the reference program's by a relative error of at most 0.012.
Values may be sent and summed in bfloat16 or wider, within the bound.
A program may use at most 128 MiB of HBM per device.

```python
import jax
import jax.numpy as jnp

D = 16384
TOKENS = 512
LAYERS = 2
FEATURES = 8192


def block_scale(key, dims, pieces, least, largest):
    def one(axis_at, blocks):
        steps = jax.random.uniform(jax.random.fold_in(jax.random.fold_in(key, 6), axis_at), (blocks,), jnp.float32, least / len(pieces), largest / len(pieces))
        return jnp.repeat(jnp.exp(steps), dims[axis_at] // blocks).reshape((-1,) + (1,) * (len(dims) - axis_at - 1))

    loudness = one(*pieces[0])
    for cut in pieces[1:]:
        loudness = loudness * one(*cut)
    return loudness


def gaussian(key, extent, deviation, bound, split=(), held_as=jnp.bfloat16):
    values = jax.random.normal(key, extent, jnp.float32) * deviation
    if len(split) > 0:
        values = block_scale(key, extent, split, -0.22, 0.18) * values
    return jnp.clip(values, min=-bound, max=bound).astype(held_as)


def setup_inputs(seed: int = 0) -> dict:
    streams_of = jax.random.split(jax.random.key(seed), 6)
    return {
        "resid": gaussian(streams_of[0], (TOKENS, LAYERS, D), 1.0, 6.0, ((2, 4),)),
        "enc_weight": gaussian(streams_of[1], (LAYERS, D, FEATURES), (LAYERS * D) ** -0.5, 0.03125, ((1, 4), (2, 32))),
        "enc_bias": jnp.clip(jax.random.uniform(streams_of[2], (FEATURES,), jnp.float32, -1.0, 1.0) * block_scale(streams_of[2], (FEATURES,), ((0, 32),), -0.4, 0.0), -1.0, 1.0),
        "dec_weight": gaussian(streams_of[3], (FEATURES, LAYERS, D), (FEATURES // 2) ** -0.5, 0.09375, ((0, 32), (2, 4))),
        "dec_bias": jnp.clip(jax.random.uniform(streams_of[4], (LAYERS, D), jnp.float32, -1.0, 1.0) * block_scale(streams_of[4], (LAYERS, D), ((1, 4),), -0.4, 0.0), -1.0, 1.0),
    }


def reference(resid, enc_weight, enc_bias, dec_weight, dec_bias):
    rows = resid.shape[0]
    flat = resid.reshape(rows, -1)
    encoder = enc_weight.reshape(flat.shape[1], -1)
    decoder = dec_weight.reshape(encoder.shape[1], -1)
    scale = 1.0 / jnp.sqrt(jnp.float32(rows))
    z = jnp.dot(flat, encoder, preferred_element_type=jnp.float32) + enc_bias[None, :]
    act = jnp.maximum(z, 0.0).astype(jnp.bfloat16)
    recon = jnp.dot(act, decoder, preferred_element_type=jnp.float32)
    err = (recon + dec_bias.reshape(1, -1) - flat.astype(jnp.float32)).astype(jnp.bfloat16)
    dec_grad = (jnp.dot(act.T, err, preferred_element_type=jnp.float32) * scale).astype(jnp.bfloat16)
    dact = jnp.dot(err, decoder.T, preferred_element_type=jnp.float32) * scale
    dz = jnp.where(z > 0, dact, 0.0).astype(jnp.bfloat16)
    enc_grad = jnp.dot(flat.T, dz, preferred_element_type=jnp.float32).astype(jnp.bfloat16)
    return (enc_grad.reshape(enc_weight.shape), dec_grad.reshape(dec_weight.shape))
```

```python
import functools
import math

import jax
import jax.numpy as jnp
from jax import lax
from jax.experimental import pallas as pl
from jax.experimental.pallas import tpu as pltpu
from jax.sharding import PartitionSpec as P

MESH = pl.DeviceIdType.MESH
F32 = jnp.float32
BF16 = jnp.bfloat16

CHUNKS = 8
BW = 256
RING = 4

Z = 0
RS1_FAR, RS1_NEAR, RS2_FAR, RS2_NEAR = 3, 7, 11, 15
XSUM = 19
AG2_NEAR, AG2_FAR, AG1_NEAR, AG1_FAR = 20, 24, 28, 32
DACT = 36
MESSAGES = 39
LOCAL = 6


def exchange_kernel(
    resid, enc, enc_bias, dec, dec_bias,
    act_out, dz_out, err_out, plain_out,
    enc_v, dec_raw, dec_v, raw, plain, own_resid, zs, zf, act_v,
    rec, far1, near1, far2, near2, xs, xr, err, own_d, ds, dr,
    send_sems, recv_sems, copy_sems, err_sems, plain_sems,
):
    layer, cut = lax.axis_index("layer"), lax.axis_index("cuts")
    x_hi, py, pz = layer // 16, (layer // 4) % 4, layer % 4
    rows = resid.shape[0]
    n = CHUNKS
    tile = rows // n
    half = tile // 2
    width = resid.shape[2]
    scale = 1.0 / math.sqrt(rows)

    def at(hi, y, z):
        return (hi * 16 + y * 4 + z, cut)

    def hop(axis, by):
        if axis == 0:
            return at(x_hi, (py + by) % 4, pz)
        return at(x_hi, py, (pz + by) % 4)

    across = at(1 - x_hi, py, pz)

    def mate(k):
        low = (cut + (k + 1) % 2) % 2
        high = (cut // 2 + (k + 1) // 2) % 2
        return high * 2 + low

    first = (py, pz)
    second = (pz, py)

    def send(m, c, src, dst, device):
        pltpu.make_async_remote_copy(
            src_ref=src, dst_ref=dst, send_sem=send_sems.at[c, m], recv_sem=recv_sems.at[c, m],
            device_id=device, device_id_type=MESH,
        ).start()

    def copy_of(m, c, ref):
        return pltpu.make_async_remote_copy(
            src_ref=ref, dst_ref=ref, send_sem=send_sems.at[c, m], recv_sem=recv_sems.at[c, m],
            device_id=across, device_id_type=MESH,
        )

    def landed(m, c, ref):
        copy_of(m, c, ref).wait_recv()

    def load_raw(c):
        return pltpu.make_async_copy(
            resid.at[pl.ds(c * tile, tile)], raw.at[c % 2], copy_sems.at[c % 2]
        )

    load_enc = pltpu.make_async_copy(enc, enc_v, copy_sems.at[2])
    load_dec = pltpu.make_async_copy(dec, dec_raw, copy_sems.at[3])

    def save_plain(c):
        return pltpu.make_async_copy(
            plain.at[c % 2], plain_out.at[:, pl.ds(c * tile, tile)], plain_sems.at[c % 2]
        )

    def save_err(c):
        return pltpu.make_async_copy(
            err.at[c], err_out.at[:, :, pl.ds(c * tile, tile)], err_sems.at[c]
        )

    load_raw(0).start()
    load_enc.start()
    load_dec.start()
    load_raw(1).start()

    barrier = pltpu.get_barrier_semaphore()
    peers = [hop(a, by) for a in (0, 1) for by in (1, 3)] + [across]
    peers += [(layer, mate(k)) for k in range(3)]
    for peer in peers:
        pl.semaphore_signal(barrier, inc=1, device_id=peer, device_id_type=MESH)
    pl.semaphore_wait(barrier, len(peers))

    def encode(c):
        load_raw(c).wait()
        slot = c % 2

        @pl.when(c >= 2)
        def _():
            save_plain(c - 2).wait()

        def split(i, carry):
            s = pl.ds(pl.multiple_of(i * 16, 16), 16)
            for l in range(2):
                plain[slot, l, s, :] = raw[slot, s, l, :]
            return carry

        lax.fori_loop(0, tile // 16, split, 0)

        @pl.when(c + 2 < n)
        def _():
            load_raw(c + 2).start()

        save_plain(c).start()

        @pl.when(c == 0)
        def _():
            load_enc.wait()

        def mul(i, acc):
            for l in range(2):
                for u in range(2):
                    k = pl.ds(pl.multiple_of((2 * i + u) * BW, BW), BW)
                    acc += jnp.dot(plain[slot, l, :, k], enc_v[l, k, :], preferred_element_type=F32)
            return acc

        acc = lax.fori_loop(0, width // (2 * BW), mul, jnp.zeros((tile, enc.shape[2]), F32))
        zs[c, cut] = acc
        for k in range(3):
            send(Z + k, c, zs.at[c, cut], zs.at[c, cut], (layer, mate(k)))
        for h in range(2):
            b = (4 * first[h] + second[h]) * BW
            own_resid[c, h] = plain[slot, h, :, pl.ds(pl.multiple_of(b, BW), BW)]

    def split_dec():
        load_dec.wait()

        def split(i, carry):
            s = pl.ds(pl.multiple_of(i * 16, 16), 16)
            for l in range(2):
                dec_v[l, s, :] = dec_raw[s, l, :]
            return carry

        lax.fori_loop(0, dec.shape[0] // 16, split, 0)

    def decode(c):
        for k in range(3):
            landed(Z + k, c, zs.at[c, mate(k)])
        z = zs[c, 0] + zs[c, 1] + zs[c, 2] + zs[c, 3] + enc_bias[...]
        zf[c] = z
        act = jnp.maximum(z, 0.0).astype(BF16)
        act_v[c] = act

        def mul(i, carry):
            for h in range(2):
                q = (first[h] + 2 + i) % RING
                for j in range(4):
                    b = 4 * q + j
                    cols = pl.ds(pl.multiple_of(b * BW, BW), BW)
                    rec[c, h, b] = jnp.dot(
                        act, dec_v[h, :, cols], preferred_element_type=F32
                    ).astype(BF16)
            return carry

        mul(0, 0)
        for h in range(2):
            q = (first[h] + 2) % RING
            for d in range(2):
                send(
                    RS1_FAR + 2 * h + d, c,
                    rec.at[c, h, pl.ds(4 * q, 4), pl.ds(d * half, half)], far1.at[c, h, d],
                    hop(h, 1 + 2 * d),
                )
        lax.fori_loop(1, 4, mul, 0)

    def rs1_relay(c):
        for h in range(2):
            for d in range(2):
                landed(RS1_FAR + 2 * h + d, c, far1.at[c, h, d])
                q = (first[h] + 1 + 2 * d) % RING
                rs = slice(d * half, (d + 1) * half)
                for k in range(4):
                    mine = rec[c, h, 4 * q + k, rs, :].astype(F32)
                    rec[c, h, 4 * q + k, rs, :] = (mine + far1[c, h, d, k].astype(F32)).astype(BF16)
                send(
                    RS1_NEAR + 2 * h + d, c, rec.at[c, h, pl.ds(4 * q, 4)], near1.at[c, h, d],
                    hop(h, 1 + 2 * d),
                )

    def rs1_sum(c):
        for h in range(2):
            for d in range(2):
                landed(RS1_NEAR + 2 * h + d, c, near1.at[c, h, d])
            p, q = first[h], (second[h] + 2) % RING
            for k in range(4):
                total = rec[c, h, 4 * p + k].astype(F32) + near1[c, h, 0, k].astype(F32)
                rec[c, h, 4 * p + k] = (total + near1[c, h, 1, k].astype(F32)).astype(BF16)
            for d in range(2):
                send(
                    RS2_FAR + 2 * h + d, c, rec.at[c, h, 4 * p + q, pl.ds(d * half, half)],
                    far2.at[c, h, d], hop(1 - h, 1 + 2 * d),
                )

    def rs2_relay(c):
        for h in range(2):
            for d in range(2):
                landed(RS2_FAR + 2 * h + d, c, far2.at[c, h, d])
                b = 4 * first[h] + (second[h] + 1 + 2 * d) % RING
                rs = slice(d * half, (d + 1) * half)
                mine = rec[c, h, b, rs, :].astype(F32)
                rec[c, h, b, rs, :] = (mine + far2[c, h, d].astype(F32)).astype(BF16)
                send(
                    RS2_NEAR + 2 * h + d, c, rec.at[c, h, b], near2.at[c, h, d],
                    hop(1 - h, 1 + 2 * d),
                )

    def rs2_sum(c):
        for h in range(2):
            for d in range(2):
                landed(RS2_NEAR + 2 * h + d, c, near2.at[c, h, d])
            b = 4 * first[h] + second[h]
            total = rec[c, h, b].astype(F32) + near2[c, h, 0].astype(F32)
            xs[c, h] = (total + near2[c, h, 1].astype(F32)).astype(BF16)
        send(XSUM, c, xs.at[c], xr.at[c], across)

    def error(c):
        landed(XSUM, c, xr.at[c])
        for h in range(2):
            b = 4 * first[h] + second[h]
            cols = pl.ds(pl.multiple_of(b * BW, BW), BW)
            recon = xs[c, h].astype(F32) + xr[c, h].astype(F32)
            value = recon + dec_bias[h : h + 1, cols] - own_resid[c, h].astype(F32)
            err[c, h, b] = value.astype(BF16)
            for d in range(2):
                send(
                    AG2_NEAR + 2 * h + d, c, err.at[c, h, b], err.at[c, h, b],
                    hop(1 - h, 1 + 2 * d),
                )

    def ag2_relay(c):
        for h in range(2):
            for d in range(2):
                b = 4 * first[h] + (second[h] + 3 + 2 * d) % RING
                landed(AG2_NEAR + 2 * h + d, c, err.at[c, h, b])
                part = err.at[c, h, b, pl.ds(d * half, half)]
                send(AG2_FAR + 2 * h + d, c, part, part, hop(1 - h, 1 + 2 * d))

    def ag1_start(c):
        for h in range(2):
            b = 4 * first[h] + (second[h] + 2) % RING
            for d in range(2):
                landed(AG2_FAR + 2 * h + d, c, err.at[c, h, b, pl.ds(d * half, half)])
            piece = err.at[c, h, pl.ds(4 * first[h], 4)]
            for d in range(2):
                send(AG1_NEAR + 2 * h + d, c, piece, piece, hop(h, 1 + 2 * d))

    def ag1_relay(c):
        for h in range(2):
            for d in range(2):
                q = (first[h] + 3 + 2 * d) % RING
                landed(AG1_NEAR + 2 * h + d, c, err.at[c, h, pl.ds(4 * q, 4)])
                part = err.at[c, h, pl.ds(4 * q, 4), pl.ds(d * half, half)]
                send(AG1_FAR + 2 * h + d, c, part, part, hop(h, 1 + 2 * d))

    def back(c):
        for h in range(2):
            q = (first[h] + 2) % RING
            for d in range(2):
                landed(
                    AG1_FAR + 2 * h + d, c, err.at[c, h, pl.ds(4 * q, 4), pl.ds(d * half, half)]
                )
        save_err(c).start()

        def mul(i, acc):
            for h in range(2):
                for j in range(4):
                    b = 4 * i + j
                    cols = pl.ds(pl.multiple_of(b * BW, BW), BW)
                    acc += lax.dot_general(
                        err[c, h, b], dec_v[h, :, cols], (((1,), (1,)), ((), ())),
                        preferred_element_type=F32,
                    )
            return acc

        acc = lax.fori_loop(0, 4, mul, jnp.zeros((tile, dec.shape[0]), F32))
        own_d[c] = acc
        ds[c] = acc.astype(BF16)
        for k in range(3):
            send(DACT + k, c, ds.at[c], dr.at[c, k], (layer, mate(k)))

    def mask(c):
        for k in range(3):
            landed(DACT + k, c, dr.at[c, k])
        total = own_d[c] + dr[c, 0].astype(F32) + dr[c, 1].astype(F32) + dr[c, 2].astype(F32)
        dz_out[c] = jnp.where(zf[c] > 0, total * scale, 0.0).astype(BF16)
        act_out[c] = act_v[c]

    stages = [
        encode, decode, rs1_relay, rs1_sum, rs2_relay, rs2_sum, error, ag2_relay, ag1_start,
        ag1_relay, back, mask,
    ]

    def step(t, carry):
        for lag in reversed(range(len(stages))):
            c = t - lag

            @pl.when((c >= 0) & (c < n))
            def _():
                stages[lag](c)

            if lag == 0:

                @pl.when(t == 0)
                def _():
                    split_dec()

        return carry

    lax.fori_loop(0, n + len(stages) - 1, step, 0)

    def finish(c, carry):
        for k in range(3):
            copy_of(Z + k, c, zs.at[c, cut]).wait_send()
            copy_of(DACT + k, c, ds.at[c]).wait_send()
        for i in range(4):
            h, d = i // 2, i % 2
            copy_of(RS1_FAR + i, c, far1.at[c, h, d]).wait_send()
            copy_of(RS1_NEAR + i, c, near1.at[c, h, d]).wait_send()
            copy_of(RS2_FAR + i, c, far2.at[c, h, d]).wait_send()
            copy_of(RS2_NEAR + i, c, near2.at[c, h, d]).wait_send()
            copy_of(AG2_NEAR + i, c, near2.at[c, h, d]).wait_send()
            copy_of(AG2_FAR + i, c, far2.at[c, h, d]).wait_send()
            copy_of(AG1_NEAR + i, c, near1.at[c, h, d]).wait_send()
            copy_of(AG1_FAR + i, c, far1.at[c, h, d]).wait_send()
        copy_of(XSUM, c, xs.at[c]).wait_send()
        save_err(c).wait()
        return carry

    lax.fori_loop(0, n, finish, 0)
    save_plain(n - 2).wait()
    save_plain(n - 1).wait()


def exchange(resid, enc, enc_bias, dec, dec_bias):
    rows, _, width = resid.shape
    feats = enc.shape[2]
    n, tile = CHUNKS, rows // CHUNKS
    half, blocks = tile // 2, width // BW
    anyspace = pl.BlockSpec(memory_space=pl.ANY)
    vmem = pl.BlockSpec(memory_space=pltpu.VMEM)
    return pl.pallas_call(
        exchange_kernel,
        out_shape=(
            jax.ShapeDtypeStruct((n, tile, feats), BF16),
            jax.ShapeDtypeStruct((n, tile, feats), BF16),
            jax.ShapeDtypeStruct((2, blocks, rows, BW), BF16),
            jax.ShapeDtypeStruct((2, rows, width), BF16),
        ),
        in_specs=[anyspace, anyspace, vmem, anyspace, vmem],
        out_specs=(vmem, vmem, anyspace, anyspace),
        scratch_shapes=[
            pltpu.VMEM((2, width, feats), BF16),
            pltpu.VMEM((feats, 2, width), BF16),
            pltpu.VMEM((2, feats, width), BF16),
            pltpu.VMEM((2, tile, 2, width), BF16),
            pltpu.VMEM((2, 2, tile, width), BF16),
            pltpu.VMEM((n, 2, tile, BW), BF16),
            pltpu.VMEM((n, 4, tile, feats), F32),
            pltpu.VMEM((n, tile, feats), F32),
            pltpu.VMEM((n, tile, feats), BF16),
            pltpu.VMEM((n, 2, blocks, tile, BW), BF16),
            pltpu.VMEM((n, 2, 2, 4, half, BW), BF16),
            pltpu.VMEM((n, 2, 2, 4, tile, BW), BF16),
            pltpu.VMEM((n, 2, 2, half, BW), BF16),
            pltpu.VMEM((n, 2, 2, tile, BW), BF16),
            pltpu.VMEM((n, 2, tile, BW), BF16),
            pltpu.VMEM((n, 2, tile, BW), BF16),
            pltpu.VMEM((n, 2, blocks, tile, BW), BF16),
            pltpu.VMEM((n, tile, feats), F32),
            pltpu.VMEM((n, tile, feats), BF16),
            pltpu.VMEM((n, 3, tile, feats), BF16),
            pltpu.SemaphoreType.DMA((n, MESSAGES)),
            pltpu.SemaphoreType.DMA((n, MESSAGES)),
            pltpu.SemaphoreType.DMA((4,)),
            pltpu.SemaphoreType.DMA((n,)),
            pltpu.SemaphoreType.DMA((2,)),
        ],
        compiler_params=pltpu.CompilerParams(
            collective_id=0, has_side_effects=True, vmem_limit_bytes=60 * 2**20
        ),
        name="exchange",
    )(resid, enc, enc_bias.reshape(1, feats), dec, dec_bias)


def grads_kernel(scale, act, dz, err, plain, enc_grad, dec_grad, act_t, dz_t):
    @pl.when(pl.program_id(0) == 0)
    def _():
        act_t[...] = act[...].T
        dz_t[...] = dz[...].T

    for h in range(2):
        grad = jnp.dot(act_t[...], err[h, 0], preferred_element_type=F32) * scale
        dec_grad[:, h, :] = grad.astype(BF16)
        flipped = jnp.dot(dz_t[...], plain[h], preferred_element_type=F32)
        enc_grad[h] = flipped.astype(BF16).T


def grads(act, dz, err, plain):
    _, rows, width = plain.shape
    feats = act.shape[1]
    full = pl.BlockSpec((rows, feats), lambda b: (0, 0))
    return pl.pallas_call(
        functools.partial(grads_kernel, 1.0 / math.sqrt(rows)),
        grid=(width // BW,),
        out_shape=(
            jax.ShapeDtypeStruct((2, width, feats), BF16),
            jax.ShapeDtypeStruct((feats, 2, width), BF16),
        ),
        in_specs=[
            full,
            full,
            pl.BlockSpec((2, 1, rows, BW), lambda b: (0, b, 0, 0)),
            pl.BlockSpec((2, rows, BW), lambda b: (0, 0, b)),
        ],
        out_specs=(
            pl.BlockSpec((2, BW, feats), lambda b: (0, b, 0)),
            pl.BlockSpec((feats, 2, BW), lambda b: (0, 0, b)),
        ),
        scratch_shapes=[pltpu.VMEM((feats, rows), BF16), pltpu.VMEM((feats, rows), BF16)],
        name="grads",
    )(act, dz, err, plain)


def per_device(resid, enc_weight, enc_bias, dec_weight, dec_bias):
    rows = resid.shape[0]
    act, dz, err, plain = exchange(resid, enc_weight, enc_bias, dec_weight, dec_bias)
    return grads(act.reshape(rows, -1), dz.reshape(rows, -1), err, plain)


def solution(mesh):
    placed = (
        P(None, None, "cuts"),
        P(None, "cuts", "layer"),
        P("layer"),
        P("layer", None, "cuts"),
        P(None, "cuts"),
    )
    return jax.shard_map(
        per_device,
        mesh=mesh,
        in_specs=placed,
        out_specs=(P(None, "cuts", "layer"), P("layer", None, "cuts")),
        check_vma=False,
    )
```

```python
import functools
import math

import jax
import jax.numpy as jnp
from jax import lax
from jax.experimental import pallas as pl
from jax.experimental.pallas import tpu as pltpu
from jax.sharding import PartitionSpec as P

MESH = pl.DeviceIdType.MESH
F32 = jnp.float32
BF16 = jnp.bfloat16

CHUNKS = 8
BW = 256
RING = 4

Z = 0
RS1_FAR, RS1_NEAR, RS2_FAR, RS2_NEAR = 3, 7, 11, 15
XSUM = 19
AG2_NEAR, AG2_FAR, AG1_NEAR, AG1_FAR = 20, 24, 28, 32
DACT = 36
MESSAGES = 39
LOCAL = 6


def exchange_kernel(
    resid, enc, enc_bias, dec, dec_bias,
    act_out, dz_out, err_out, plain_out,
    enc_v, dec_raw, dec_v, raw, plain, own_resid, zs, zf, act_v,
    rec, far1, near1, far2, near2, xs, xr, err, own_d, ds, dr,
    send_sems, recv_sems, copy_sems, err_sems, plain_sems,
):
    layer, cut = lax.axis_index("layer"), lax.axis_index("cuts")
    x_hi, py, pz = layer // 16, (layer // 4) % 4, layer % 4
    rows = resid.shape[0]
    n = CHUNKS
    tile = rows // n
    half = tile // 2
    width = resid.shape[2]
    scale = 1.0 / math.sqrt(rows)

    def at(hi, y, z):
        return (hi * 16 + y * 4 + z, cut)

    def hop(axis, by):
        if axis == 0:
            return at(x_hi, (py + by) % 4, pz)
        return at(x_hi, py, (pz + by) % 4)

    across = at(1 - x_hi, py, pz)

    def mate(k):
        low = (cut + (k + 1) % 2) % 2
        high = (cut // 2 + (k + 1) // 2) % 2
        return high * 2 + low

    first = (py, pz)
    second = (pz, py)

    def send(m, c, src, dst, device):
        pltpu.make_async_remote_copy(
            src_ref=src, dst_ref=dst, send_sem=send_sems.at[c, m], recv_sem=recv_sems.at[c, m],
            device_id=device, device_id_type=MESH,
        ).start()

    def copy_of(m, c, ref):
        return pltpu.make_async_remote_copy(
            src_ref=ref, dst_ref=ref, send_sem=send_sems.at[c, m], recv_sem=recv_sems.at[c, m],
            device_id=across, device_id_type=MESH,
        )

    def landed(m, c, ref):
        copy_of(m, c, ref).wait_recv()

    def load_raw(c):
        return pltpu.make_async_copy(
            resid.at[pl.ds(c * tile, tile)], raw.at[c % 2], copy_sems.at[c % 2]
        )

    load_enc = pltpu.make_async_copy(enc, enc_v, copy_sems.at[2])
    load_dec = pltpu.make_async_copy(dec, dec_raw, copy_sems.at[3])

    def save_plain(c):
        return pltpu.make_async_copy(
            plain.at[c % 2], plain_out.at[:, pl.ds(c * tile, tile)], plain_sems.at[c % 2]
        )

    def save_err(c):
        return pltpu.make_async_copy(
            err.at[c], err_out.at[:, :, pl.ds(c * tile, tile)], err_sems.at[c]
        )

    load_raw(0).start()
    load_enc.start()
    load_dec.start()
    load_raw(1).start()

    barrier = pltpu.get_barrier_semaphore()
    peers = [hop(a, by) for a in (0, 1) for by in (1, 3)] + [across]
    peers += [(layer, mate(k)) for k in range(3)]
    for peer in peers:
        pl.semaphore_signal(barrier, inc=1, device_id=peer, device_id_type=MESH)
    pl.semaphore_wait(barrier, len(peers))

    def encode(c):
        load_raw(c).wait()
        slot = c % 2

        @pl.when(c >= 2)
        def _():
            save_plain(c - 2).wait()

        def split(i, carry):
            s = pl.ds(pl.multiple_of(i * 16, 16), 16)
            plain[slot, :, s, :] = jnp.swapaxes(raw[slot, s], 0, 1)
            return carry

        lax.fori_loop(0, tile // 16, split, 0)

        @pl.when(c + 2 < n)
        def _():
            load_raw(c + 2).start()

        save_plain(c).start()

        @pl.when(c == 0)
        def _():
            load_enc.wait()

        def mul(i, acc):
            for l in range(2):
                for u in range(2):
                    k = pl.ds(pl.multiple_of((2 * i + u) * BW, BW), BW)
                    acc += jnp.dot(plain[slot, l, :, k], enc_v[l, k, :], preferred_element_type=F32)
            return acc

        acc = lax.fori_loop(0, width // (2 * BW), mul, jnp.zeros((tile, enc.shape[2]), F32))
        zs[c, cut] = acc
        for k in range(3):
            send(Z + k, c, zs.at[c, cut], zs.at[c, cut], (layer, mate(k)))
        for h in range(2):
            b = (4 * first[h] + second[h]) * BW
            own_resid[c, h] = plain[slot, h, :, pl.ds(pl.multiple_of(b, BW), BW)]

    def split_dec():
        load_dec.wait()

        def split(i, carry):
            s = pl.ds(pl.multiple_of(i * 16, 16), 16)
            dec_v[:, s, :] = jnp.swapaxes(dec_raw[s], 0, 1)
            return carry

        lax.fori_loop(0, dec.shape[0] // 16, split, 0)

    def decode(c):
        for k in range(3):
            landed(Z + k, c, zs.at[c, mate(k)])
        z = zs[c, 0] + zs[c, 1] + zs[c, 2] + zs[c, 3] + enc_bias[...]
        zf[c] = z
        act = jnp.maximum(z, 0.0).astype(BF16)
        act_v[c] = act

        def mul(i, carry):
            for h in range(2):
                q = (first[h] + 2 + i) % RING
                for j in range(4):
                    b = 4 * q + j
                    cols = pl.ds(pl.multiple_of(b * BW, BW), BW)
                    rec[c, h, b] = jnp.dot(
                        act, dec_v[h, :, cols], preferred_element_type=F32
                    ).astype(BF16)
            return carry

        mul(0, 0)
        for h in range(2):
            q = (first[h] + 2) % RING
            for d in range(2):
                send(
                    RS1_FAR + 2 * h + d, c,
                    rec.at[c, h, pl.ds(4 * q, 4), pl.ds(d * half, half)], far1.at[c, h, d],
                    hop(h, 1 + 2 * d),
                )
        lax.fori_loop(1, 4, mul, 0)

    def rs1_relay(c):
        for h in range(2):
            for d in range(2):
                landed(RS1_FAR + 2 * h + d, c, far1.at[c, h, d])
                q = (first[h] + 1 + 2 * d) % RING
                rs = slice(d * half, (d + 1) * half)
                for k in range(4):
                    mine = rec[c, h, 4 * q + k, rs, :].astype(F32)
                    rec[c, h, 4 * q + k, rs, :] = (mine + far1[c, h, d, k].astype(F32)).astype(BF16)
                send(
                    RS1_NEAR + 2 * h + d, c, rec.at[c, h, pl.ds(4 * q, 4)], near1.at[c, h, d],
                    hop(h, 1 + 2 * d),
                )

    def rs1_sum(c):
        for h in range(2):
            for d in range(2):
                landed(RS1_NEAR + 2 * h + d, c, near1.at[c, h, d])
            p, q = first[h], (second[h] + 2) % RING
            for k in range(4):
                total = rec[c, h, 4 * p + k].astype(F32) + near1[c, h, 0, k].astype(F32)
                rec[c, h, 4 * p + k] = (total + near1[c, h, 1, k].astype(F32)).astype(BF16)
            for d in range(2):
                send(
                    RS2_FAR + 2 * h + d, c, rec.at[c, h, 4 * p + q, pl.ds(d * half, half)],
                    far2.at[c, h, d], hop(1 - h, 1 + 2 * d),
                )

    def rs2_relay(c):
        for h in range(2):
            for d in range(2):
                landed(RS2_FAR + 2 * h + d, c, far2.at[c, h, d])
                b = 4 * first[h] + (second[h] + 1 + 2 * d) % RING
                rs = slice(d * half, (d + 1) * half)
                mine = rec[c, h, b, rs, :].astype(F32)
                rec[c, h, b, rs, :] = (mine + far2[c, h, d].astype(F32)).astype(BF16)
                send(
                    RS2_NEAR + 2 * h + d, c, rec.at[c, h, b], near2.at[c, h, d],
                    hop(1 - h, 1 + 2 * d),
                )

    def rs2_sum(c):
        for h in range(2):
            for d in range(2):
                landed(RS2_NEAR + 2 * h + d, c, near2.at[c, h, d])
            b = 4 * first[h] + second[h]
            total = rec[c, h, b].astype(F32) + near2[c, h, 0].astype(F32)
            xs[c, h] = (total + near2[c, h, 1].astype(F32)).astype(BF16)
        send(XSUM, c, xs.at[c], xr.at[c], across)

    def error(c):
        landed(XSUM, c, xr.at[c])
        for h in range(2):
            b = 4 * first[h] + second[h]
            cols = pl.ds(pl.multiple_of(b * BW, BW), BW)
            recon = xs[c, h].astype(F32) + xr[c, h].astype(F32)
            value = recon + dec_bias[h : h + 1, cols] - own_resid[c, h].astype(F32)
            err[c, h, b] = value.astype(BF16)
            for d in range(2):
                send(
                    AG2_NEAR + 2 * h + d, c, err.at[c, h, b], err.at[c, h, b],
                    hop(1 - h, 1 + 2 * d),
                )

    def ag2_relay(c):
        for h in range(2):
            for d in range(2):
                b = 4 * first[h] + (second[h] + 3 + 2 * d) % RING
                landed(AG2_NEAR + 2 * h + d, c, err.at[c, h, b])
                part = err.at[c, h, b, pl.ds(d * half, half)]
                send(AG2_FAR + 2 * h + d, c, part, part, hop(1 - h, 1 + 2 * d))

    def ag1_start(c):
        for h in range(2):
            b = 4 * first[h] + (second[h] + 2) % RING
            for d in range(2):
                landed(AG2_FAR + 2 * h + d, c, err.at[c, h, b, pl.ds(d * half, half)])
            piece = err.at[c, h, pl.ds(4 * first[h], 4)]
            for d in range(2):
                send(AG1_NEAR + 2 * h + d, c, piece, piece, hop(h, 1 + 2 * d))

    def ag1_relay(c):
        for h in range(2):
            for d in range(2):
                q = (first[h] + 3 + 2 * d) % RING
                landed(AG1_NEAR + 2 * h + d, c, err.at[c, h, pl.ds(4 * q, 4)])
                part = err.at[c, h, pl.ds(4 * q, 4), pl.ds(d * half, half)]
                send(AG1_FAR + 2 * h + d, c, part, part, hop(h, 1 + 2 * d))

    def back(c):
        for h in range(2):
            q = (first[h] + 2) % RING
            for d in range(2):
                landed(
                    AG1_FAR + 2 * h + d, c, err.at[c, h, pl.ds(4 * q, 4), pl.ds(d * half, half)]
                )
        save_err(c).start()

        def mul(i, acc):
            for h in range(2):
                for j in range(4):
                    b = 4 * i + j
                    cols = pl.ds(pl.multiple_of(b * BW, BW), BW)
                    acc += lax.dot_general(
                        err[c, h, b], dec_v[h, :, cols], (((1,), (1,)), ((), ())),
                        preferred_element_type=F32,
                    )
            return acc

        acc = lax.fori_loop(0, 4, mul, jnp.zeros((tile, dec.shape[0]), F32))
        own_d[c] = acc
        ds[c] = acc.astype(BF16)
        for k in range(3):
            send(DACT + k, c, ds.at[c], dr.at[c, k], (layer, mate(k)))

    def mask(c):
        for k in range(3):
            landed(DACT + k, c, dr.at[c, k])
        total = own_d[c] + dr[c, 0].astype(F32) + dr[c, 1].astype(F32) + dr[c, 2].astype(F32)
        dz_out[c] = jnp.where(zf[c] > 0, total * scale, 0.0).astype(BF16)
        act_out[c] = act_v[c]

    stages = [
        encode, decode, rs1_relay, rs1_sum, rs2_relay, rs2_sum, error, ag2_relay, ag1_start,
        ag1_relay, back, mask,
    ]

    ORDER = range(len(stages))

    def step(t, carry):
        for lag in ORDER:
            c = t - lag

            @pl.when((c >= 0) & (c < n))
            def _():
                stages[lag](c)

            if lag == 0:

                @pl.when(t == 0)
                def _():
                    split_dec()

        return carry

    lax.fori_loop(0, n + len(stages) - 1, step, 0)

    def finish(c, carry):
        for k in range(3):
            copy_of(Z + k, c, zs.at[c, cut]).wait_send()
            copy_of(DACT + k, c, ds.at[c]).wait_send()
        for i in range(4):
            h, d = i // 2, i % 2
            copy_of(RS1_FAR + i, c, far1.at[c, h, d]).wait_send()
            copy_of(RS1_NEAR + i, c, near1.at[c, h, d]).wait_send()
            copy_of(RS2_FAR + i, c, far2.at[c, h, d]).wait_send()
            copy_of(RS2_NEAR + i, c, near2.at[c, h, d]).wait_send()
            copy_of(AG2_NEAR + i, c, near2.at[c, h, d]).wait_send()
            copy_of(AG2_FAR + i, c, far2.at[c, h, d]).wait_send()
            copy_of(AG1_NEAR + i, c, near1.at[c, h, d]).wait_send()
            copy_of(AG1_FAR + i, c, far1.at[c, h, d]).wait_send()
        copy_of(XSUM, c, xs.at[c]).wait_send()
        save_err(c).wait()
        return carry

    lax.fori_loop(0, n, finish, 0)
    save_plain(n - 2).wait()
    save_plain(n - 1).wait()


def exchange(resid, enc, enc_bias, dec, dec_bias):
    rows, _, width = resid.shape
    feats = enc.shape[2]
    n, tile = CHUNKS, rows // CHUNKS
    half, blocks = tile // 2, width // BW
    anyspace = pl.BlockSpec(memory_space=pl.ANY)
    vmem = pl.BlockSpec(memory_space=pltpu.VMEM)
    return pl.pallas_call(
        exchange_kernel,
        out_shape=(
            jax.ShapeDtypeStruct((n, tile, feats), BF16),
            jax.ShapeDtypeStruct((n, tile, feats), BF16),
            jax.ShapeDtypeStruct((2, blocks, rows, BW), BF16),
            jax.ShapeDtypeStruct((2, rows, width), BF16),
        ),
        in_specs=[anyspace, anyspace, vmem, anyspace, vmem],
        out_specs=(vmem, vmem, anyspace, anyspace),
        scratch_shapes=[
            pltpu.VMEM((2, width, feats), BF16),
            pltpu.VMEM((feats, 2, width), BF16),
            pltpu.VMEM((2, feats, width), BF16),
            pltpu.VMEM((2, tile, 2, width), BF16),
            pltpu.VMEM((2, 2, tile, width), BF16),
            pltpu.VMEM((n, 2, tile, BW), BF16),
            pltpu.VMEM((n, 4, tile, feats), F32),
            pltpu.VMEM((n, tile, feats), F32),
            pltpu.VMEM((n, tile, feats), BF16),
            pltpu.VMEM((n, 2, blocks, tile, BW), BF16),
            pltpu.VMEM((n, 2, 2, 4, half, BW), BF16),
            pltpu.VMEM((n, 2, 2, 4, tile, BW), BF16),
            pltpu.VMEM((n, 2, 2, half, BW), BF16),
            pltpu.VMEM((n, 2, 2, tile, BW), BF16),
            pltpu.VMEM((n, 2, tile, BW), BF16),
            pltpu.VMEM((n, 2, tile, BW), BF16),
            pltpu.VMEM((n, 2, blocks, tile, BW), BF16),
            pltpu.VMEM((n, tile, feats), F32),
            pltpu.VMEM((n, tile, feats), BF16),
            pltpu.VMEM((n, 3, tile, feats), BF16),
            pltpu.SemaphoreType.DMA((n, MESSAGES)),
            pltpu.SemaphoreType.DMA((n, MESSAGES)),
            pltpu.SemaphoreType.DMA((4,)),
            pltpu.SemaphoreType.DMA((n,)),
            pltpu.SemaphoreType.DMA((2,)),
        ],
        compiler_params=pltpu.CompilerParams(
            collective_id=0, has_side_effects=True, vmem_limit_bytes=60 * 2**20
        ),
        name="exchange",
    )(resid, enc, enc_bias.reshape(1, feats), dec, dec_bias)


def grads_kernel(scale, act, dz, err, plain, enc_grad, dec_grad, act_t, dz_t):
    @pl.when(pl.program_id(0) == 0)
    def _():
        act_t[...] = act[...].T
        dz_t[...] = dz[...].T

    for h in range(2):
        for u in range(err.shape[1]):
            s = slice(u * BW, (u + 1) * BW)
            grad = jnp.dot(act_t[...], err[h, u], preferred_element_type=F32) * scale
            dec_grad[:, h, s] = grad.astype(BF16)
            flipped = jnp.dot(dz_t[...], plain[h, :, s], preferred_element_type=F32)
            enc_grad[h, s] = flipped.astype(BF16).T


def grads(act, dz, err, plain):
    _, rows, width = plain.shape
    feats = act.shape[1]
    full = pl.BlockSpec((rows, feats), lambda b: (0, 0))
    return pl.pallas_call(
        functools.partial(grads_kernel, 1.0 / math.sqrt(rows)),
        grid=(width // (4 * BW),),
        out_shape=(
            jax.ShapeDtypeStruct((2, width, feats), BF16),
            jax.ShapeDtypeStruct((feats, 2, width), BF16),
        ),
        in_specs=[
            full,
            full,
            pl.BlockSpec((2, 4, rows, BW), lambda b: (0, b, 0, 0)),
            pl.BlockSpec((2, rows, 4 * BW), lambda b: (0, 0, b)),
        ],
        out_specs=(
            pl.BlockSpec((2, 4 * BW, feats), lambda b: (0, b, 0)),
            pl.BlockSpec((feats, 2, 4 * BW), lambda b: (0, 0, b)),
        ),
        scratch_shapes=[pltpu.VMEM((feats, rows), BF16), pltpu.VMEM((feats, rows), BF16)],
        name="grads",
    )(act, dz, err, plain)


def per_device(resid, enc_weight, enc_bias, dec_weight, dec_bias):
    rows = resid.shape[0]
    act, dz, err, plain = exchange(resid, enc_weight, enc_bias, dec_weight, dec_bias)
    return grads(act.reshape(rows, -1), dz.reshape(rows, -1), err, plain)


def solution(mesh):
    placed = (
        P(None, None, "cuts"),
        P(None, "cuts", "layer"),
        P("layer"),
        P("layer", None, "cuts"),
        P(None, "cuts"),
    )
    return jax.shard_map(
        per_device,
        mesh=mesh,
        in_specs=placed,
        out_specs=(P(None, "cuts", "layer"), P("layer", None, "cuts")),
        check_vma=False,
    )
```

```python
import math

import jax
import jax.numpy as jnp
from jax import lax
from jax.experimental import pallas as pl
from jax.experimental.pallas import tpu as pltpu
from jax.sharding import PartitionSpec as P

MESH = pl.DeviceIdType.MESH
F32 = jnp.float32
BF16 = jnp.bfloat16

CHUNKS = 8
BW = 256
PART = 1024
VMEM_LIMIT = 97 * 2**19
RING = 4

Z = 0
RS1_FAR, RS1_NEAR, RS2_FAR, RS2_NEAR = 3, 7, 11, 15
XSUM = 19
AG2_NEAR, AG2_FAR, AG1_NEAR, AG1_FAR = 20, 24, 28, 32
DACT = 36
MESSAGES = 39


def exchange_kernel(
    resid, enc, enc_bias, dec, dec_bias,
    enc_v, dec_grad,
    dec_raw, dec_v, raw, plain, own_resid, zs, zf, act_v, dz_v, act_t, dz_t,
    rec, far1, near1, far2, near2, xs, xr, err, own_d, ds, dr,
    send_sems, recv_sems, copy_sems, out_sems, bias_v, dec_bias_v,
):
    layer, cut = lax.axis_index("layer"), lax.axis_index("cuts")
    x_hi, py, pz = layer // 16, (layer // 4) % 4, layer % 4
    rows = resid.shape[0]
    n = CHUNKS
    tile = rows // n
    half = tile // 2
    width = resid.shape[2]
    scale = 1.0 / math.sqrt(rows)

    def at(hi, y, z):
        return (hi * 16 + y * 4 + z, cut)

    def hop(axis, by):
        if axis == 0:
            return at(x_hi, (py + by) % 4, pz)
        return at(x_hi, py, (pz + by) % 4)

    across = at(1 - x_hi, py, pz)

    def mate(k):
        low = (cut + (k + 1) % 2) % 2
        high = (cut // 2 + (k + 1) // 2) % 2
        return high * 2 + low

    first = (py, pz)
    second = (pz, py)

    def send(m, c, src, dst, device):
        pltpu.make_async_remote_copy(
            src_ref=src, dst_ref=dst, send_sem=send_sems.at[c, m], recv_sem=recv_sems.at[c, m],
            device_id=device, device_id_type=MESH,
        ).start()

    def copy_of(m, c, ref):
        return pltpu.make_async_remote_copy(
            src_ref=ref, dst_ref=ref, send_sem=send_sems.at[c, m], recv_sem=recv_sems.at[c, m],
            device_id=across, device_id_type=MESH,
        )

    def landed(m, c, ref):
        copy_of(m, c, ref).wait_recv()

    def load_raw(c):
        return pltpu.make_async_copy(
            resid.at[pl.ds(c * tile, tile)], raw.at[c % 2], copy_sems.at[c % 2]
        )

    def load_enc(i):
        part = pl.ds(pl.multiple_of(i * (width // 2), width // 2), width // 2)
        return pltpu.make_async_copy(enc.at[:, part], enc_v.at[:, part], copy_sems.at[4 + i])

    load_dec = pltpu.make_async_copy(dec, dec_raw, copy_sems.at[3])

    def save_dec(i):
        part = pl.ds(pl.multiple_of(i * PART, PART), PART)
        return pltpu.make_async_copy(dec_raw.at[:, :, part], dec_grad.at[:, :, part], out_sems.at[i])

    load_bias = pltpu.make_async_copy(enc_bias, bias_v, copy_sems.at[2])
    load_dec_bias = pltpu.make_async_copy(dec_bias, dec_bias_v, copy_sems.at[6])

    load_raw(0).start()
    load_enc(0).start()
    load_enc(1).start()

    barrier = pltpu.get_barrier_semaphore()
    peers = [hop(a, by) for a in (0, 1) for by in (1, 3)] + [across]
    peers += [(layer, mate(k)) for k in range(3)]
    for peer in peers:
        pl.semaphore_signal(barrier, inc=1, device_id=peer, device_id_type=MESH)
    def encode_own(c):
        load_raw(c).wait()
        here = pl.ds(pl.multiple_of(c * tile, tile), tile)

        def split(i, carry):
            s = pl.ds(pl.multiple_of(i * 16, 16), 16)
            to = pl.ds(pl.multiple_of(c * tile + i * 16, 16), 16)
            plain[:, to, :] = jnp.swapaxes(raw[c % 2, s], 0, 1)
            return carry

        lax.fori_loop(0, tile // 16, split, 0)

        @pl.when(c + 2 < n)
        def _():
            load_raw(c + 2).start()

        per = width // (2 * BW)

        def mul(i, acc):
            @pl.when(c == 0)
            def _():
                load_enc(i).wait()

            for l in range(2):
                for u in range(per):
                    k = pl.ds(pl.multiple_of((per * i + u) * BW, BW), BW)
                    acc += jnp.dot(plain[l, here, k], enc_v[l, k, :], preferred_element_type=F32)
            return acc

        acc = lax.fori_loop(0, 2, mul, jnp.zeros((tile, enc.shape[2]), F32))

        @pl.when(c == 0)
        def _():
            load_raw(1).start()
            load_dec.start()
            load_bias.start()
            load_dec_bias.start()

        zs[c, cut] = acc

    def encode(c):
        @pl.when(c > 0)
        def _():
            encode_own(c)

        for k in range(3):
            send(Z + k, c, zs.at[c, cut], zs.at[c, cut], (layer, mate(k)))
        here = pl.ds(pl.multiple_of(c * tile, tile), tile)
        for h in range(2):
            b = (4 * first[h] + second[h]) * BW
            own_resid[c, h] = plain[h, here, pl.ds(pl.multiple_of(b, BW), BW)]

    def split_dec():
        load_dec.wait()
        load_bias.wait()
        load_dec_bias.wait()

        def split(i, carry):
            s = pl.ds(pl.multiple_of(i * 16, 16), 16)
            dec_v[:, s, :] = jnp.swapaxes(dec_raw[s], 0, 1)
            return carry

        lax.fori_loop(0, dec.shape[0] // 16, split, 0)

    def decode(c):
        for k in range(3):
            landed(Z + k, c, zs.at[c, mate(k)])
        z = zs[c, 0] + zs[c, 1] + zs[c, 2] + zs[c, 3] + bias_v[...]
        zf[c] = z
        act = jnp.maximum(z, 0.0).astype(BF16)
        act_v[c] = act

        def mul(i, carry):
            for h in range(2):
                q = (first[h] + 2 + i) % RING
                for j in range(4):
                    b = 4 * q + j
                    cols = pl.ds(pl.multiple_of(b * BW, BW), BW)
                    rec[c, h, b] = jnp.dot(
                        act, dec_v[h, :, cols], preferred_element_type=F32
                    ).astype(BF16)
            return carry

        mul(0, 0)
        for h in range(2):
            q = (first[h] + 2) % RING
            for d in range(2):
                send(
                    RS1_FAR + 2 * h + d, c,
                    rec.at[c, h, pl.ds(4 * q, 4), pl.ds(d * half, half)], far1.at[c, h, d],
                    hop(h, 1 + 2 * d),
                )
        for i in range(1, 4):
            mul(i, 0)

    def rs1_relay(c):
        for h in range(2):
            for d in range(2):
                landed(RS1_FAR + 2 * h + d, c, far1.at[c, h, d])
                q = (first[h] + 1 + 2 * d) % RING
                rs = slice(d * half, (d + 1) * half)
                for k in range(4):
                    mine = rec[c, h, 4 * q + k, rs, :].astype(F32)
                    rec[c, h, 4 * q + k, rs, :] = (mine + far1[c, h, d, k].astype(F32)).astype(BF16)
                send(
                    RS1_NEAR + 2 * h + d, c, rec.at[c, h, pl.ds(4 * q, 4)], near1.at[c, h, d],
                    hop(h, 1 + 2 * d),
                )

    def rs1_sum(c):
        for h in range(2):
            for d in range(2):
                landed(RS1_NEAR + 2 * h + d, c, near1.at[c, h, d])
            p, q = first[h], (second[h] + 2) % RING
            for k in range(4):
                total = rec[c, h, 4 * p + k].astype(F32) + near1[c, h, 0, k].astype(F32)
                rec[c, h, 4 * p + k] = (total + near1[c, h, 1, k].astype(F32)).astype(BF16)
            for d in range(2):
                send(
                    RS2_FAR + 2 * h + d, c, rec.at[c, h, 4 * p + q, pl.ds(d * half, half)],
                    far2.at[c, h, d], hop(1 - h, 1 + 2 * d),
                )

    def rs2_relay(c):
        for h in range(2):
            for d in range(2):
                landed(RS2_FAR + 2 * h + d, c, far2.at[c, h, d])
                b = 4 * first[h] + (second[h] + 1 + 2 * d) % RING
                rs = slice(d * half, (d + 1) * half)
                mine = rec[c, h, b, rs, :].astype(F32)
                rec[c, h, b, rs, :] = (mine + far2[c, h, d].astype(F32)).astype(BF16)
                send(
                    RS2_NEAR + 2 * h + d, c, rec.at[c, h, b], near2.at[c, h, d],
                    hop(1 - h, 1 + 2 * d),
                )

    def rs2_sum(c):
        for h in range(2):
            for d in range(2):
                landed(RS2_NEAR + 2 * h + d, c, near2.at[c, h, d])
            b = 4 * first[h] + second[h]
            total = rec[c, h, b].astype(F32) + near2[c, h, 0].astype(F32)
            xs[c, h] = (total + near2[c, h, 1].astype(F32)).astype(BF16)
        send(XSUM, c, xs.at[c], xr.at[c], across)

    def error(c):
        landed(XSUM, c, xr.at[c])
        for h in range(2):
            b = 4 * first[h] + second[h]
            cols = pl.ds(pl.multiple_of(b * BW, BW), BW)
            recon = xs[c, h].astype(F32) + xr[c, h].astype(F32)
            value = recon + dec_bias_v[h : h + 1, cols] - own_resid[c, h].astype(F32)
            err[c, h, b] = value.astype(BF16)
            for d in range(2):
                send(
                    AG2_NEAR + 2 * h + d, c, err.at[c, h, b], err.at[c, h, b],
                    hop(1 - h, 1 + 2 * d),
                )

    def ag2_relay(c):
        for h in range(2):
            for d in range(2):
                b = 4 * first[h] + (second[h] + 3 + 2 * d) % RING
                landed(AG2_NEAR + 2 * h + d, c, err.at[c, h, b])
                part = err.at[c, h, b, pl.ds(d * half, half)]
                send(AG2_FAR + 2 * h + d, c, part, part, hop(1 - h, 1 + 2 * d))

    def ag1_start(c):
        for h in range(2):
            b = 4 * first[h] + (second[h] + 2) % RING
            for d in range(2):
                landed(AG2_FAR + 2 * h + d, c, err.at[c, h, b, pl.ds(d * half, half)])
            piece = err.at[c, h, pl.ds(4 * first[h], 4)]
            for d in range(2):
                send(AG1_NEAR + 2 * h + d, c, piece, piece, hop(h, 1 + 2 * d))

    def ag1_relay(c):
        for h in range(2):
            for d in range(2):
                q = (first[h] + 3 + 2 * d) % RING
                landed(AG1_NEAR + 2 * h + d, c, err.at[c, h, pl.ds(4 * q, 4)])
                part = err.at[c, h, pl.ds(4 * q, 4), pl.ds(d * half, half)]
                send(AG1_FAR + 2 * h + d, c, part, part, hop(h, 1 + 2 * d))

    def back(c):
        for h in range(2):
            q = (first[h] + 2) % RING
            for d in range(2):
                landed(
                    AG1_FAR + 2 * h + d, c, err.at[c, h, pl.ds(4 * q, 4), pl.ds(d * half, half)]
                )
        def mul(i, acc):
            for h in range(2):
                for j in range(8):
                    b = 8 * i + j
                    cols = pl.ds(pl.multiple_of(b * BW, BW), BW)
                    acc += lax.dot_general(
                        err[c, h, b], dec_v[h, :, cols], (((1,), (1,)), ((), ())),
                        preferred_element_type=F32,
                    )
            return acc

        acc = lax.fori_loop(0, 2, mul, jnp.zeros((tile, dec.shape[0]), F32))
        own_d[c] = acc
        ds[c] = acc.astype(BF16)
        for k in range(3):
            send(DACT + k, c, ds.at[c], dr.at[c, k], (layer, mate(k)))

    def mask(c):
        for k in range(3):
            landed(DACT + k, c, dr.at[c, k])
        total = own_d[c] + dr[c, 0].astype(F32) + dr[c, 1].astype(F32) + dr[c, 2].astype(F32)
        dz_v[c] = jnp.where(zf[c] > 0, total * scale, 0.0).astype(BF16)

    def finish(c):
        for k in range(3):
            copy_of(Z + k, c, zs.at[c, cut]).wait_send()
            copy_of(DACT + k, c, ds.at[c]).wait_send()
        for i in range(4):
            h, d = i // 2, i % 2
            copy_of(RS1_FAR + i, c, far1.at[c, h, d]).wait_send()
            copy_of(RS1_NEAR + i, c, near1.at[c, h, d]).wait_send()
            copy_of(RS2_FAR + i, c, far2.at[c, h, d]).wait_send()
            copy_of(RS2_NEAR + i, c, near2.at[c, h, d]).wait_send()
            copy_of(AG2_NEAR + i, c, near2.at[c, h, d]).wait_send()
            copy_of(AG2_FAR + i, c, far2.at[c, h, d]).wait_send()
            copy_of(AG1_NEAR + i, c, near1.at[c, h, d]).wait_send()
            copy_of(AG1_FAR + i, c, far1.at[c, h, d]).wait_send()
        copy_of(XSUM, c, xs.at[c]).wait_send()

    def make_dec_grad():
        act_t[...] = act_v[...].reshape(rows, -1).T

        def mul(i, carry):
            for u in range(PART // BW):
                b = (PART // BW) * i + u
                cols = pl.ds(pl.multiple_of(b * BW, BW), BW)
                both = []
                for h in range(2):
                    tall = jnp.concatenate([err[c, h, b] for c in range(n)], axis=0)
                    grad = jnp.dot(act_t[...], tall, preferred_element_type=F32) * scale
                    both.append(grad.astype(BF16))
                dec_raw[:, :, cols] = jnp.swapaxes(jnp.stack(both), 0, 1)
            save_dec(i).start()
            return carry

        lax.fori_loop(0, width // PART, mul, 0)

    def make_enc_grad():
        dz_t[...] = dz_v[...].reshape(rows, -1).T

        def mul(i, carry):
            for u in range(PART // BW):
                b = (PART // BW) * i + u
                cols = pl.ds(pl.multiple_of(b * BW, BW), BW)
                for h in range(2):
                    flipped = jnp.dot(dz_t[...], plain[h, :, cols], preferred_element_type=F32)
                    enc_v[h, cols, :] = flipped.astype(BF16).T
            return carry

        lax.fori_loop(0, width // PART, mul, 0)

    stages = [
        encode, decode, rs1_relay, rs1_sum, rs2_relay, rs2_sum, error, ag2_relay, ag1_start,
        ag1_relay, back, mask, finish,
    ]

    ORDER = range(len(stages))

    def step(t, carry):
        for lag in ORDER:
            c = t - lag

            @pl.when((c >= 0) & (c < n))
            def _():
                stages[lag](c)

            if lag == 0:

                @pl.when(t == 0)
                def _():
                    split_dec()

        @pl.when(t == n - 1 + stages.index(back))
        def _():
            make_dec_grad()

        return carry

    encode_own(0)
    pl.semaphore_wait(barrier, len(peers))
    lax.fori_loop(0, n + len(stages) - 1, step, 0)
    make_enc_grad()
    for i in range(width // PART):
        save_dec(i).wait()


def exchange(resid, enc, enc_bias, dec, dec_bias):
    rows, _, width = resid.shape
    feats = enc.shape[2]
    n, tile = CHUNKS, rows // CHUNKS
    half, blocks = tile // 2, width // BW
    hbm = pl.BlockSpec(memory_space=pltpu.HBM)
    vmem = pl.BlockSpec(memory_space=pltpu.VMEM)
    return pl.pallas_call(
        exchange_kernel,
        out_shape=(
            jax.ShapeDtypeStruct((2, width, feats), BF16),
            jax.ShapeDtypeStruct((feats, 2, width), BF16),
        ),
        in_specs=[hbm] * 5,
        out_specs=(vmem, hbm),
        scratch_shapes=[
            pltpu.VMEM((feats, 2, width), BF16),
            pltpu.VMEM((2, feats, width), BF16),
            pltpu.VMEM((2, tile, 2, width), BF16),
            pltpu.VMEM((2, rows, width), BF16),
            pltpu.VMEM((n, 2, tile, BW), BF16),
            pltpu.VMEM((n, 4, tile, feats), F32),
            pltpu.VMEM((n, tile, feats), F32),
            pltpu.VMEM((n, tile, feats), BF16),
            pltpu.VMEM((n, tile, feats), BF16),
            pltpu.VMEM((feats, rows), BF16),
            pltpu.VMEM((feats, rows), BF16),
            pltpu.VMEM((n, 2, blocks, tile, BW), BF16),
            pltpu.VMEM((n, 2, 2, 4, half, BW), BF16),
            pltpu.VMEM((n, 2, 2, 4, tile, BW), BF16),
            pltpu.VMEM((n, 2, 2, half, BW), BF16),
            pltpu.VMEM((n, 2, 2, tile, BW), BF16),
            pltpu.VMEM((n, 2, tile, BW), BF16),
            pltpu.VMEM((n, 2, tile, BW), BF16),
            pltpu.VMEM((n, 2, blocks, tile, BW), BF16),
            pltpu.VMEM((n, tile, feats), F32),
            pltpu.VMEM((n, tile, feats), BF16),
            pltpu.VMEM((n, 3, tile, feats), BF16),
            pltpu.SemaphoreType.DMA((n, MESSAGES)),
            pltpu.SemaphoreType.DMA((n, MESSAGES)),
            pltpu.SemaphoreType.DMA((7,)),
            pltpu.SemaphoreType.DMA((width // PART,)),
            pltpu.VMEM((1, feats), F32),
            pltpu.VMEM((2, width), F32),
        ],
        compiler_params=pltpu.CompilerParams(
            collective_id=0, has_side_effects=True, vmem_limit_bytes=VMEM_LIMIT
        ),
        name="exchange",
    )(resid, enc, enc_bias.reshape(1, feats), dec, dec_bias)


def per_device(resid, enc_weight, enc_bias, dec_weight, dec_bias):
    return exchange(resid, enc_weight, enc_bias, dec_weight, dec_bias)


def solution(mesh):
    placed = (
        P(None, None, "cuts"),
        P(None, "cuts", "layer"),
        P("layer"),
        P("layer", None, "cuts"),
        P(None, "cuts"),
    )
    return jax.shard_map(
        per_device,
        mesh=mesh,
        in_specs=placed,
        out_specs=(P(None, "cuts", "layer"), P("layer", None, "cuts")),
        check_vma=False,
    )
```

```python
import math

import jax
import jax.numpy as jnp
from jax import lax
from jax.experimental import pallas as pl
from jax.experimental.pallas import tpu as pltpu
from jax.sharding import PartitionSpec as P

MESH = pl.DeviceIdType.MESH
F32 = jnp.float32
BF16 = jnp.bfloat16

CHUNKS = 8
BW = 256
PART = 1024
VMEM_LIMIT = 97 * 2**19
RING = 4

Z = 0
RS1_FAR, RS1_NEAR, RS2_FAR, RS2_NEAR = 3, 7, 11, 15
XSUM = 19
AG2_NEAR, AG2_FAR, AG1_NEAR, AG1_FAR = 20, 24, 28, 32
DACT = 36
MESSAGES = 39


def exchange_kernel(
    resid, enc, enc_bias, dec, dec_bias,
    enc_v, dec_grad,
    dec_raw, dec_v, raw, plain, own_resid, zs, zf, act_v, dz_v, act_t, dz_t,
    rec, far1, near1, far2, near2, xs, xr, err, own_d, ds, dr,
    send_sems, recv_sems, copy_sems, out_sems, bias_v, dec_bias_v,
):
    layer, cut = lax.axis_index("layer"), lax.axis_index("cuts")
    x_hi, py, pz = layer // 16, (layer // 4) % 4, layer % 4
    rows = resid.shape[0]
    n = CHUNKS
    tile = rows // n
    half = tile // 2
    width = resid.shape[2]
    scale = 1.0 / math.sqrt(rows)

    def at(hi, y, z):
        return (hi * 16 + y * 4 + z, cut)

    def hop(axis, by):
        if axis == 0:
            return at(x_hi, (py + by) % 4, pz)
        return at(x_hi, py, (pz + by) % 4)

    across = at(1 - x_hi, py, pz)

    def mate(k):
        low = (cut + (k + 1) % 2) % 2
        high = (cut // 2 + (k + 1) // 2) % 2
        return high * 2 + low

    first = (py, pz)
    second = (pz, py)

    def send(m, c, src, dst, device):
        pltpu.make_async_remote_copy(
            src_ref=src, dst_ref=dst, send_sem=send_sems.at[c, m], recv_sem=recv_sems.at[c, m],
            device_id=device, device_id_type=MESH,
        ).start()

    def copy_of(m, c, ref):
        return pltpu.make_async_remote_copy(
            src_ref=ref, dst_ref=ref, send_sem=send_sems.at[c, m], recv_sem=recv_sems.at[c, m],
            device_id=across, device_id_type=MESH,
        )

    def landed(m, c, ref):
        copy_of(m, c, ref).wait_recv()

    def load_raw(c):
        return pltpu.make_async_copy(
            resid.at[pl.ds(c * tile, tile)], raw.at[c % 2], copy_sems.at[c % 2]
        )

    def load_enc(i):
        part = pl.ds(pl.multiple_of(i * (width // 2), width // 2), width // 2)
        return pltpu.make_async_copy(enc.at[:, part], enc_v.at[:, part], copy_sems.at[4 + i])

    load_dec = pltpu.make_async_copy(dec, dec_raw, copy_sems.at[3])

    def save_dec(i):
        part = pl.ds(pl.multiple_of(i * PART, PART), PART)
        return pltpu.make_async_copy(dec_raw.at[:, :, part], dec_grad.at[:, :, part], out_sems.at[i])

    load_bias = pltpu.make_async_copy(enc_bias, bias_v, copy_sems.at[2])
    load_dec_bias = pltpu.make_async_copy(dec_bias, dec_bias_v, copy_sems.at[6])

    load_raw(0).start()
    load_enc(0).start()
    load_enc(1).start()

    barrier = pltpu.get_barrier_semaphore()
    peers = [hop(a, by) for a in (0, 1) for by in (1, 3)] + [across]
    peers += [(layer, mate(k)) for k in range(3)]
    for peer in peers:
        pl.semaphore_signal(barrier, inc=1, device_id=peer, device_id_type=MESH)
    def encode_own(c):
        load_raw(c).wait()
        here = pl.ds(pl.multiple_of(c * tile, tile), tile)

        def split(i, carry):
            s = pl.ds(pl.multiple_of(i * 16, 16), 16)
            to = pl.ds(pl.multiple_of(c * tile + i * 16, 16), 16)
            plain[:, to, :] = jnp.swapaxes(raw[c % 2, s], 0, 1)
            return carry

        lax.fori_loop(0, tile // 16, split, 0)

        @pl.when(c + 2 < n)
        def _():
            load_raw(c + 2).start()

        per = width // (2 * BW)

        def mul(i, acc):
            @pl.when(c == 0)
            def _():
                load_enc(i).wait()

            for l in range(2):
                for u in range(per):
                    k = pl.ds(pl.multiple_of((per * i + u) * BW, BW), BW)
                    acc += jnp.dot(plain[l, here, k], enc_v[l, k, :], preferred_element_type=F32)
            return acc

        acc = lax.fori_loop(0, 2, mul, jnp.zeros((tile, enc.shape[2]), F32))

        @pl.when(c == 0)
        def _():
            load_raw(1).start()
            load_dec.start()
            load_bias.start()
            load_dec_bias.start()

        zs[c, cut] = acc

    def encode(c):
        @pl.when(c > 0)
        def _():
            encode_own(c)

        for k in (1, 2, 0):
            send(Z + k, c, zs.at[c, cut], zs.at[c, cut], (layer, mate(k)))
        here = pl.ds(pl.multiple_of(c * tile, tile), tile)
        for h in range(2):
            b = (4 * first[h] + second[h]) * BW
            own_resid[c, h] = plain[h, here, pl.ds(pl.multiple_of(b, BW), BW)]

    def split_dec():
        load_dec.wait()
        load_bias.wait()
        load_dec_bias.wait()

        def split(i, carry):
            s = pl.ds(pl.multiple_of(i * 16, 16), 16)
            dec_v[:, s, :] = jnp.swapaxes(dec_raw[s], 0, 1)
            return carry

        lax.fori_loop(0, dec.shape[0] // 16, split, 0)

    def decode(c):
        for k in range(3):
            landed(Z + k, c, zs.at[c, mate(k)])
        z = zs[c, 0] + zs[c, 1] + zs[c, 2] + zs[c, 3] + bias_v[...]
        zf[c] = z
        act = jnp.maximum(z, 0.0).astype(BF16)
        act_v[c] = act

        def mul(i, carry):
            for h in range(2):
                q = (first[h] + 2 + i) % RING
                for j in range(4):
                    b = 4 * q + j
                    cols = pl.ds(pl.multiple_of(b * BW, BW), BW)
                    rec[c, h, b] = jnp.dot(
                        act, dec_v[h, :, cols], preferred_element_type=F32
                    ).astype(BF16)
            return carry

        mul(0, 0)
        for h in range(2):
            q = (first[h] + 2) % RING
            for d in range(2):
                send(
                    RS1_FAR + 2 * h + d, c,
                    rec.at[c, h, pl.ds(4 * q, 4), pl.ds(d * half, half)], far1.at[c, h, d],
                    hop(h, 1 + 2 * d),
                )
        for i in range(1, 4):
            mul(i, 0)

    def rs1_relay(c):
        for h in range(2):
            for d in range(2):
                landed(RS1_FAR + 2 * h + d, c, far1.at[c, h, d])
                q = (first[h] + 1 + 2 * d) % RING
                rs = slice(d * half, (d + 1) * half)
                for k in range(4):
                    mine = rec[c, h, 4 * q + k, rs, :].astype(F32)
                    rec[c, h, 4 * q + k, rs, :] = (mine + far1[c, h, d, k].astype(F32)).astype(BF16)
                send(
                    RS1_NEAR + 2 * h + d, c, rec.at[c, h, pl.ds(4 * q, 4)], near1.at[c, h, d],
                    hop(h, 1 + 2 * d),
                )

    def rs1_sum(c):
        for h in range(2):
            for d in range(2):
                landed(RS1_NEAR + 2 * h + d, c, near1.at[c, h, d])
            p, q = first[h], (second[h] + 2) % RING
            for k in range(4):
                total = rec[c, h, 4 * p + k].astype(F32) + near1[c, h, 0, k].astype(F32)
                rec[c, h, 4 * p + k] = (total + near1[c, h, 1, k].astype(F32)).astype(BF16)
            for d in range(2):
                send(
                    RS2_FAR + 2 * h + d, c, rec.at[c, h, 4 * p + q, pl.ds(d * half, half)],
                    far2.at[c, h, d], hop(1 - h, 1 + 2 * d),
                )

    def rs2_relay(c):
        for h in range(2):
            for d in range(2):
                landed(RS2_FAR + 2 * h + d, c, far2.at[c, h, d])
                b = 4 * first[h] + (second[h] + 1 + 2 * d) % RING
                rs = slice(d * half, (d + 1) * half)
                mine = rec[c, h, b, rs, :].astype(F32)
                rec[c, h, b, rs, :] = (mine + far2[c, h, d].astype(F32)).astype(BF16)
                send(
                    RS2_NEAR + 2 * h + d, c, rec.at[c, h, b], near2.at[c, h, d],
                    hop(1 - h, 1 + 2 * d),
                )

    def rs2_sum(c):
        for h in range(2):
            for d in range(2):
                landed(RS2_NEAR + 2 * h + d, c, near2.at[c, h, d])
            b = 4 * first[h] + second[h]
            total = rec[c, h, b].astype(F32) + near2[c, h, 0].astype(F32)
            xs[c, h] = (total + near2[c, h, 1].astype(F32)).astype(BF16)
        send(XSUM, c, xs.at[c], xr.at[c], across)

    def error(c):
        landed(XSUM, c, xr.at[c])
        for h in range(2):
            b = 4 * first[h] + second[h]
            cols = pl.ds(pl.multiple_of(b * BW, BW), BW)
            recon = xs[c, h].astype(F32) + xr[c, h].astype(F32)
            value = recon + dec_bias_v[h : h + 1, cols] - own_resid[c, h].astype(F32)
            err[c, h, b] = value.astype(BF16)
            for d in range(2):
                send(
                    AG2_NEAR + 2 * h + d, c, err.at[c, h, b], err.at[c, h, b],
                    hop(1 - h, 1 + 2 * d),
                )

    def ag2_relay(c):
        for h in range(2):
            for d in range(2):
                b = 4 * first[h] + (second[h] + 3 + 2 * d) % RING
                landed(AG2_NEAR + 2 * h + d, c, err.at[c, h, b])
                part = err.at[c, h, b, pl.ds(d * half, half)]
                send(AG2_FAR + 2 * h + d, c, part, part, hop(1 - h, 1 + 2 * d))

    def ag1_start(c):
        for h in range(2):
            b = 4 * first[h] + (second[h] + 2) % RING
            for d in range(2):
                landed(AG2_FAR + 2 * h + d, c, err.at[c, h, b, pl.ds(d * half, half)])
            piece = err.at[c, h, pl.ds(4 * first[h], 4)]
            for d in range(2):
                send(AG1_NEAR + 2 * h + d, c, piece, piece, hop(h, 1 + 2 * d))

    def ag1_relay(c):
        for h in range(2):
            for d in range(2):
                q = (first[h] + 3 + 2 * d) % RING
                landed(AG1_NEAR + 2 * h + d, c, err.at[c, h, pl.ds(4 * q, 4)])
                part = err.at[c, h, pl.ds(4 * q, 4), pl.ds(d * half, half)]
                send(AG1_FAR + 2 * h + d, c, part, part, hop(h, 1 + 2 * d))

    def back(c):
        for h in range(2):
            q = (first[h] + 2) % RING
            for d in range(2):
                landed(
                    AG1_FAR + 2 * h + d, c, err.at[c, h, pl.ds(4 * q, 4), pl.ds(d * half, half)]
                )
        def mul(i, acc):
            for h in range(2):
                for j in range(8):
                    b = 8 * i + j
                    cols = pl.ds(pl.multiple_of(b * BW, BW), BW)
                    acc += lax.dot_general(
                        err[c, h, b], dec_v[h, :, cols], (((1,), (1,)), ((), ())),
                        preferred_element_type=F32,
                    )
            return acc

        acc = lax.fori_loop(0, 2, mul, jnp.zeros((tile, dec.shape[0]), F32))
        own_d[c] = acc
        ds[c] = acc.astype(BF16)
        for k in (1, 2, 0):
            send(DACT + k, c, ds.at[c], dr.at[c, k], (layer, mate(k)))

    def mask(c):
        for k in range(3):
            landed(DACT + k, c, dr.at[c, k])
        total = own_d[c] + dr[c, 0].astype(F32) + dr[c, 1].astype(F32) + dr[c, 2].astype(F32)
        dz_v[c] = jnp.where(zf[c] > 0, total * scale, 0.0).astype(BF16)

    def finish(c):
        for k in range(3):
            copy_of(Z + k, c, zs.at[c, cut]).wait_send()
            copy_of(DACT + k, c, ds.at[c]).wait_send()
        for i in range(4):
            h, d = i // 2, i % 2
            copy_of(RS1_FAR + i, c, far1.at[c, h, d]).wait_send()
            copy_of(RS1_NEAR + i, c, near1.at[c, h, d]).wait_send()
            copy_of(RS2_FAR + i, c, far2.at[c, h, d]).wait_send()
            copy_of(RS2_NEAR + i, c, near2.at[c, h, d]).wait_send()
            copy_of(AG2_NEAR + i, c, near2.at[c, h, d]).wait_send()
            copy_of(AG2_FAR + i, c, far2.at[c, h, d]).wait_send()
            copy_of(AG1_NEAR + i, c, near1.at[c, h, d]).wait_send()
            copy_of(AG1_FAR + i, c, far1.at[c, h, d]).wait_send()
        copy_of(XSUM, c, xs.at[c]).wait_send()

    def make_dec_grad():
        def mul(i, carry):
            for u in range(PART // BW):
                b = (PART // BW) * i + u
                cols = pl.ds(pl.multiple_of(b * BW, BW), BW)
                both = []
                for h in range(2):
                    tall = jnp.concatenate([err[c, h, b] for c in range(n)], axis=0)
                    grad = jnp.dot(act_t[...], tall, preferred_element_type=F32) * scale
                    both.append(grad.astype(BF16))
                dec_raw[:, :, cols] = jnp.swapaxes(jnp.stack(both), 0, 1)
            save_dec(i).start()
            return carry

        lax.fori_loop(0, width // PART, mul, 0)

    def make_enc_grad():
        dz_t[...] = dz_v[...].reshape(rows, -1).T

        def mul(i, carry):
            for u in range(PART // BW):
                b = (PART // BW) * i + u
                cols = pl.ds(pl.multiple_of(b * BW, BW), BW)
                for h in range(2):
                    flipped = jnp.dot(dz_t[...], plain[h, :, cols], preferred_element_type=F32)
                    enc_v[h, cols, :] = flipped.astype(BF16).T
            return carry

        lax.fori_loop(0, width // PART, mul, 0)

    stages = [
        encode, decode, rs1_relay, rs1_sum, rs2_relay, rs2_sum, error, ag2_relay, ag1_start,
        ag1_relay, back, mask, finish,
    ]

    ORDER = range(len(stages))

    def step(t, carry):
        for lag in ORDER:
            c = t - lag

            @pl.when((c >= 0) & (c < n))
            def _():
                stages[lag](c)

            if lag == 0:

                @pl.when(t == 0)
                def _():
                    split_dec()

        @pl.when(t == n + stages.index(decode) + 3)
        def _():
            act_t[...] = act_v[...].reshape(rows, -1).T

        @pl.when(t == n - 1 + stages.index(back))
        def _():
            make_dec_grad()

        return carry

    encode_own(0)
    pl.semaphore_wait(barrier, len(peers))
    lax.fori_loop(0, n + len(stages) - 1, step, 0)
    make_enc_grad()
    for i in range(width // PART):
        save_dec(i).wait()


def exchange(resid, enc, enc_bias, dec, dec_bias):
    rows, _, width = resid.shape
    feats = enc.shape[2]
    n, tile = CHUNKS, rows // CHUNKS
    half, blocks = tile // 2, width // BW
    hbm = pl.BlockSpec(memory_space=pltpu.HBM)
    vmem = pl.BlockSpec(memory_space=pltpu.VMEM)
    return pl.pallas_call(
        exchange_kernel,
        out_shape=(
            jax.ShapeDtypeStruct((2, width, feats), BF16),
            jax.ShapeDtypeStruct((feats, 2, width), BF16),
        ),
        in_specs=[hbm] * 5,
        out_specs=(vmem, hbm),
        scratch_shapes=[
            pltpu.VMEM((feats, 2, width), BF16),
            pltpu.VMEM((2, feats, width), BF16),
            pltpu.VMEM((2, tile, 2, width), BF16),
            pltpu.VMEM((2, rows, width), BF16),
            pltpu.VMEM((n, 2, tile, BW), BF16),
            pltpu.VMEM((n, 4, tile, feats), F32),
            pltpu.VMEM((n, tile, feats), F32),
            pltpu.VMEM((n, tile, feats), BF16),
            pltpu.VMEM((n, tile, feats), BF16),
            pltpu.VMEM((feats, rows), BF16),
            pltpu.VMEM((feats, rows), BF16),
            pltpu.VMEM((n, 2, blocks, tile, BW), BF16),
            pltpu.VMEM((n, 2, 2, 4, half, BW), BF16),
            pltpu.VMEM((n, 2, 2, 4, tile, BW), BF16),
            pltpu.VMEM((n, 2, 2, half, BW), BF16),
            pltpu.VMEM((n, 2, 2, tile, BW), BF16),
            pltpu.VMEM((n, 2, tile, BW), BF16),
            pltpu.VMEM((n, 2, tile, BW), BF16),
            pltpu.VMEM((n, 2, blocks, tile, BW), BF16),
            pltpu.VMEM((n, tile, feats), F32),
            pltpu.VMEM((n, tile, feats), BF16),
            pltpu.VMEM((n, 3, tile, feats), BF16),
            pltpu.SemaphoreType.DMA((n, MESSAGES)),
            pltpu.SemaphoreType.DMA((n, MESSAGES)),
            pltpu.SemaphoreType.DMA((7,)),
            pltpu.SemaphoreType.DMA((width // PART,)),
            pltpu.VMEM((1, feats), F32),
            pltpu.VMEM((2, width), F32),
        ],
        compiler_params=pltpu.CompilerParams(
            collective_id=0, has_side_effects=True, vmem_limit_bytes=VMEM_LIMIT
        ),
        name="exchange",
    )(resid, enc, enc_bias.reshape(1, feats), dec, dec_bias)


def per_device(resid, enc_weight, enc_bias, dec_weight, dec_bias):
    return exchange(resid, enc_weight, enc_bias, dec_weight, dec_bias)


def solution(mesh):
    placed = (
        P(None, None, "cuts"),
        P(None, "cuts", "layer"),
        P("layer"),
        P("layer", None, "cuts"),
        P(None, "cuts"),
    )
    return jax.shard_map(
        per_device,
        mesh=mesh,
        in_specs=placed,
        out_specs=(P(None, "cuts", "layer"), P("layer", None, "cuts")),
        check_vma=False,
    )
```
